64 devices in a mesh: dp: 4 (over x, y), tp: 16 (over z, core).
Axes of the slice: x: 2, y: 2, z: 8, core: 2. Of those that a mesh axis runs over, the one named last changes fastest.
The devices are a block of a 4x4x8 slice.
Arguments:
- x: bfloat16 [256, 4608], P('dp'), parts along dimension 0
- k_cache: bfloat16 [256, 2048, 16, 128], P('dp', None, 'tp'), parts along dimension 0
- v_cache: bfloat16 [256, 2048, 16, 128], P('dp', None, 'tp'), parts along dimension 0
- gain_a: bfloat16 [4608], replicated
- wq: bfloat16 [4608, 4096], P(None, 'tp')
- wo: bfloat16 [4096, 4608], P('tp')
- gain_m: bfloat16 [4608], replicated
- w_gate: bfloat16 [4608, 36864], P(None, 'tp')
- w_up: bfloat16 [4608, 36864], P(None, 'tp')
- w_down: bfloat16 [36864, 4608], P('tp')
Outputs:
- output: bfloat16 [256, 4608], P('dp'), parts along dimension 0
There are 4 independent parts. The reference program is written for one: setup_inputs(seed, part) draws one part's arguments, and reference() takes and returns one part's arrays. A program takes and returns all parts, laid end to end along the dimension named above; an argument that names none is the same for every part.
All inputs are finite; a program needn't handle non-finite values.
Results may differ from the reference program's by a relative error of at most 0.0171.
Values are sent between devices in bfloat16 or wider.
A program may use at most 768 MiB of HBM per device.

```python
import jax
import jax.numpy as jnp
from jax import lax

BATCH = 64
CACHE = 2048
D = 4608
HEADS = 32
KV_HEADS = 16
HEAD = 128
FF = 36864
THETA = 10000


def setup_inputs(seed: int = 0, part: int = 0) -> dict:
    kx, kc, kw, kn, kq, ko, km, kg, ku, kd = jax.random.split(jax.random.key(seed), 10)
    kx, kc, kw = (jax.random.fold_in(k, part) for k in (kx, kc, kw))

    def weights(key, rows, columns):
        return jax.random.normal(key, (rows, columns), jnp.float32) * rows**-0.5

    drawn = {
        "x": jax.random.normal(kx, (BATCH, D), jnp.float32),
        "k_cache": 2 * jax.random.normal(kc, (BATCH, CACHE, KV_HEADS, HEAD), jnp.float32),
        "v_cache": 4 * jax.random.normal(kw, (BATCH, CACHE, KV_HEADS, HEAD), jnp.float32),
        "gain_a": 1 + 0.1 * jax.random.normal(kn, (D,), jnp.float32),
        "wq": 2 * weights(kq, D, HEADS * HEAD),
        "wo": weights(ko, HEADS * HEAD, D),
        "gain_m": 1 + 0.1 * jax.random.normal(km, (D,), jnp.float32),
        "w_gate": weights(kg, D, FF),
        "w_up": weights(ku, D, FF),
        "w_down": 2 * weights(kd, FF, D),
    }
    return {k: v.astype(jnp.bfloat16) for k, v in drawn.items()}


def normed(x, gain):
    wide = x.astype(jnp.float32)
    scale = lax.rsqrt(jnp.mean(wide * wide, -1, keepdims=True) + 1e-6)
    return (wide * scale * gain.astype(jnp.float32)).astype(jnp.bfloat16)


def turned(t, place, theta):
    half = t.shape[-1] // 2
    angle = place.astype(jnp.float32)[:, None] * theta ** (-jnp.arange(half, dtype=jnp.float32) / half)
    cos, sin = jnp.cos(angle)[:, None], jnp.sin(angle)[:, None]
    a, b = t[..., :half].astype(jnp.float32), t[..., half:].astype(jnp.float32)
    return jnp.concatenate([a * cos - b * sin, b * cos + a * sin], -1).astype(jnp.bfloat16)


def matmul(a, w):
    return jnp.dot(a, w, preferred_element_type=jnp.float32).astype(jnp.bfloat16)


def einsum(form, a, b):
    return jnp.einsum(form, a.astype(jnp.float32), b.astype(jnp.float32))


def seen_by(a, wq, k_cache, v_cache, head, theta):
    batch, cache, kv_heads = k_cache.shape[:3]
    place = jnp.full((batch,), cache - 1)
    q = turned(matmul(a, wq).reshape(batch, -1, head), place, theta).reshape(batch, kv_heads, -1, head)
    scores = einsum("bgsd,bugd->bgsu", q, k_cache) * head**-0.5
    weights = jax.nn.softmax(scores, -1).astype(jnp.bfloat16)
    return einsum("bgsu,bugd->bgsd", weights, v_cache).astype(jnp.bfloat16).reshape(batch, -1)


def hidden_of(b, w_gate, w_up):
    gate = jnp.dot(b, w_gate, preferred_element_type=jnp.float32)
    up = jnp.dot(b, w_up, preferred_element_type=jnp.float32)
    return (jax.nn.silu(gate) * up).astype(jnp.bfloat16)


def reference(x, k_cache, v_cache, gain_a, wq, wo, gain_m, w_gate, w_up, w_down):
    seen = seen_by(normed(x, gain_a), wq, k_cache, v_cache, HEAD, THETA)
    h = (x.astype(jnp.float32) + jnp.dot(seen, wo, preferred_element_type=jnp.float32)).astype(jnp.bfloat16)
    hidden = hidden_of(normed(h, gain_m), w_gate, w_up)
    return (h.astype(jnp.float32) + jnp.dot(hidden, w_down, preferred_element_type=jnp.float32)).astype(jnp.bfloat16)
```

```python
import functools

import jax
import jax.numpy as jnp
import numpy as np
from jax import lax
from jax.experimental import pallas as pl
from jax.experimental.pallas import tpu as pltpu
from jax.sharding import PartitionSpec as P

HEAD = 128
THETA = 10000
CHUNK = 256
RING = 40
BLOCK = 8
CORES = 2
F32, BF16 = jnp.float32, jnp.bfloat16
MESH = pl.DeviceIdType.MESH


def turns(place):
    half = HEAD // 2
    angle = np.float64(place) * np.float64(THETA) ** (-np.arange(half) / half)
    cos, sin = np.cos(angle), np.sin(angle)
    return np.stack([np.concatenate([cos, cos]), np.concatenate([-sin, sin])]).astype(np.float32)


def layer(chips, x, k, v, gains, wq, wo, wg, wu, wd, rot, out, slots, wq_v, wo_v, gains_v, rot_v, xb, hb, bb, qb, hid,
          own1, ds1, dr1, ss1, sr1, own2, ds2, dr2, ss2, sr2, yb,
          ring_sem, misc_sem, d1s, d1r, r1s, r1r, a1s, a1r, f1s, f1r, d2s, d2r, r2s, r2r, a2s, a2r, f2s, f2r, out_sem):
    d = wq.shape[0]
    half = d // CORES
    cache = k.shape[1]
    hidden = wd.shape[0]
    pairs = BLOCK // 2
    per_block = 2 * pairs
    n_kv = chips * per_block
    n_up = hidden // CHUNK
    n_down = half // CHUNK
    gate_rows = d // 2
    first_down = n_kv + 4 * n_up
    total = first_down + 2 * n_down

    me = lax.axis_index("tp")
    z, c = me // CORES, lax.rem(me, CORES)
    other = 1 - c
    offsets = [chips // 2]
    for far in range(chips // 2 - 1, 0, -1):
        offsets += [far, -far]

    def device(chip, core):
        return {"tp": chip * CORES + core}

    def away(off):
        return lax.rem(z + off + chips, chips)

    def slot_of(off):
        return (-off) % chips - 1

    def dest(j):
        far = chips // 2 - (j + 1) // 2
        return lax.rem(z + jnp.where(lax.rem(j, 2) == 1, far, chips - far), chips)

    def remote(src, dst, send, recv, chip, core):
        return pltpu.make_async_remote_copy(src_ref=src, dst_ref=dst, send_sem=send, recv_sem=recv, device_id=device(chip, core), device_id_type=MESH)

    def arrived(ref, sem):
        pltpu.make_async_copy(ref, ref, sem).wait()

    def two_rows(src, row0, rows, col0, s):
        for e in range(2):
            n = rows // 2
            pltpu.make_async_copy(
                src.at[pl.ds(row0 + e * n, n), pl.ds(pl.multiple_of(col0, CHUNK), CHUNK)], slots.at[s, pl.ds(e * n, n), :], ring_sem.at[s, e]
            ).start()

    def issue(i):
        s = lax.rem(i, RING)

        @pl.when(i < n_kv)
        def _():
            w = lax.rem(i, per_block)
            first = dest(i // per_block) * BLOCK + 2 * lax.rem(w, pairs)

            @pl.when(w < pairs)
            def _():
                for e in range(2):
                    pltpu.make_async_copy(k.at[first + e], slots.at[s, pl.ds(0, cache), pl.ds(e * HEAD, HEAD)], ring_sem.at[s, e]).start()

            @pl.when(w >= pairs)
            def _():
                for e in range(2):
                    pltpu.make_async_copy(v.at[first + e], slots.at[s, pl.ds(0, cache), pl.ds(e * HEAD, HEAD)], ring_sem.at[s, e]).start()

        @pl.when((i >= n_kv) & (i < first_down))
        def _():
            m = i - n_kv
            n, r = m // 4, lax.rem(m, 4)
            row0 = lax.rem(r, 2) * gate_rows

            @pl.when(r < 2)
            def _():
                two_rows(wg, row0, gate_rows, n * CHUNK, s)

            @pl.when(r >= 2)
            def _():
                two_rows(wu, row0, gate_rows, n * CHUNK, s)

        @pl.when((i >= first_down) & (i < total))
        def _():
            m = i - first_down
            core = jnp.where(lax.rem(m, 2) == 0, other, c)
            two_rows(wd, 0, hidden, core * half + (m // 2) * CHUNK, s)

    def ready_cache(s):
        for e in range(2):
            pltpu.make_async_copy(k.at[0], slots.at[s, pl.ds(0, cache), pl.ds(e * HEAD, HEAD)], ring_sem.at[s, e]).wait()

    def ready_rows(src, rows, s):
        for e in range(2):
            n = rows // 2
            pltpu.make_async_copy(src.at[pl.ds(e * n, n), pl.ds(0, CHUNK)], slots.at[s, pl.ds(e * n, n), :], ring_sem.at[s, e]).wait()

    def x_copy(a, b):
        return pltpu.make_async_copy(x.at[pl.ds(a * BLOCK, BLOCK), pl.ds(b * half, half)], xb.at[a, b], misc_sem.at[0])

    for a in range(chips):
        for b in range(CORES):
            x_copy(a, b).start()
    small = [
        pltpu.make_async_copy(gains, gains_v, misc_sem.at[1]),
        pltpu.make_async_copy(rot, rot_v, misc_sem.at[2]),
        pltpu.make_async_copy(wq, wq_v, misc_sem.at[3]),
    ]
    for copy in small:
        copy.start()
    lax.fori_loop(0, per_block, lambda i, _: (issue(i), 0)[1], 0)
    wo_copies = [
        pltpu.make_async_copy(wo.at[:, pl.ds(pl.multiple_of(core * half, CHUNK), half)], wo_v.at[e], misc_sem.at[4 + e])
        for e, core in enumerate((other, c))
    ]
    for copy in wo_copies:
        copy.start()
    lax.fori_loop(per_block, RING, lambda i, _: (issue(i), 0)[1], 0)

    barrier = pltpu.get_barrier_semaphore()
    for off in offsets:
        pl.semaphore_signal(barrier, inc=1, device_id=device(away(off), c), device_id_type=MESH)
    pl.semaphore_signal(barrier, inc=1, device_id=device(z, other), device_id_type=MESH)

    def normed(src, which):
        def two_blocks(m, _):
            rows = [[src[2 * m + a, b].astype(F32) for b in range(CORES)] for a in range(2)]
            scaled = []
            for parts in rows:
                mean = sum(jnp.sum(t * t, -1, keepdims=True) for t in parts) / d
                scale = lax.rsqrt(mean + 1e-6)
                scaled.append([t * scale * gains_v[which : which + 1, b * half : (b + 1) * half] for b, t in enumerate(parts)])
            at = pl.ds(pl.multiple_of(m * 2 * BLOCK, 2 * BLOCK), 2 * BLOCK)
            for b in range(CORES):
                bb[b, at, :] = jnp.concatenate([scaled[0][b], scaled[1][b]], 0).astype(BF16)
            return 0

        lax.fori_loop(0, chips // 2, two_blocks, 0)

    for a in range(2):
        small[a].wait()
    arrived(xb, misc_sem.at[0])
    normed(xb, 0)
    small[2].wait()
    q = jnp.dot(bb[0], wq_v[:half], preferred_element_type=F32) + jnp.dot(bb[1], wq_v[half:], preferred_element_type=F32)
    q = q.astype(BF16).astype(F32)
    turned = []
    for h in range(2):
        t = q[:, h * HEAD : (h + 1) * HEAD]
        turned.append(t * rot_v[0:1, :] + pltpu.roll(t, HEAD // 2, 1) * rot_v[1:2, :])
    for a in range(chips):
        rows = slice(a * BLOCK, (a + 1) * BLOCK)
        qb[a] = jnp.concatenate([turned[0][rows], turned[1][rows]], 0).astype(BF16)
    for copy in wo_copies:
        copy.wait()
    pl.semaphore_wait(barrier, len(offsets) + 1)

    row = lax.rem(lax.broadcasted_iota(jnp.int32, (2 * BLOCK, 2 * HEAD), 0), BLOCK)
    side = lax.broadcasted_iota(jnp.int32, (2 * BLOCK, 2 * HEAD), 1) // HEAD

    def d2d1(j):
        return remote(ds1.at[j], dr1.at[j], d1s.at[j], d1r.at[j], z, other)

    def rs1(j):
        t = dest(j)
        return remote(ss1.at[j], sr1.at[lax.rem(z - t + chips, chips) - 1], r1s.at[j], r1r, t, c)

    def pass_on(j):
        d2d1(j).wait_recv()
        ss1[j] = (own1[j] + dr1[j].astype(F32)).astype(BF16)
        rs1(j).start()

    def attend(j, _):
        base = j * per_block
        q16 = qb[dest(j)]
        wide = jnp.concatenate([q16, q16], 1)
        s = None
        for p in range(pairs):
            slot = lax.rem(base + p, RING)
            ready_cache(slot)
            mine = jnp.where(row == 2 * p + side, wide, jnp.zeros_like(wide))
            part = lax.dot_general(mine, slots[slot, :cache, :], (((1,), (1,)), ((), ())), preferred_element_type=F32)
            s = part if s is None else s + part
        s = s * HEAD**-0.5
        e = jnp.exp(s - jnp.max(s, -1, keepdims=True))
        weights = (e / jnp.sum(e, -1, keepdims=True)).astype(BF16)

        @pl.when(j > 0)
        def _():
            pass_on(j - 1)

        o = None
        for p in range(pairs):
            slot = lax.rem(base + pairs + p, RING)
            ready_cache(slot)
            part = jnp.dot(weights, slots[slot, :cache, :], preferred_element_type=F32)
            part = jnp.where(row == 2 * p + side, part, 0.0)
            o = part if o is None else o + part
        o = o[:, :HEAD] + o[:, HEAD:]
        seen = jnp.concatenate([o[:BLOCK], o[BLOCK:]], 1).astype(BF16)
        ds1[j] = jnp.dot(seen, wo_v[0], preferred_element_type=F32).astype(BF16)
        d2d1(j).start()
        own1[j] = jnp.dot(seen, wo_v[1], preferred_element_type=F32)
        lax.fori_loop(0, per_block, lambda i, _: (issue(base + RING + i), 0)[1], 0)
        return 0

    lax.fori_loop(0, chips, attend, 0)

    d2d1(chips - 1).wait_recv()
    h = own1[chips - 1] + dr1[chips - 1].astype(F32)
    arrived(sr1, r1r)
    for a in range(chips - 1):
        h = h + sr1[a].astype(F32)
    h = h + xb[z, c].astype(F32)
    hb[z, c] = h.astype(BF16)

    def ag1(i):
        off = offsets[i]
        return remote(hb.at[z, c], hb.at[z, c], a1s.at[i], a1r.at[slot_of(off)], away(off), c)

    def fw1(i, chip):
        return remote(hb.at[chip, c], hb.at[chip, c], f1s.at[i], f1r, z, other)

    for i in range(chips - 1):
        ag1(i).start()
    fw1(0, z).start()
    for i in reversed(range(chips - 1)):
        off = offsets[i]
        arrived(hb.at[away(off), c], a1r.at[off % chips - 1])
        fw1(1 + i, away(off)).start()
    arrived(hb.at[:, other], f1r)
    normed(hb, 1)

    def gated(n, _):
        base = n_kv + 4 * n
        parts = []
        for r in range(4):
            slot = lax.rem(base + r, RING)
            ready_rows(wg, gate_rows, slot)
            parts.append(jnp.dot(bb[r % 2], slots[slot, :gate_rows, :], preferred_element_type=F32))
        gate, up = parts[0] + parts[1], parts[2] + parts[3]
        hid[:, pl.ds(pl.multiple_of(n * CHUNK, CHUNK), CHUNK)] = (gate * jax.nn.sigmoid(gate) * up).astype(BF16)
        lax.fori_loop(0, 4, lambda i, _: (issue(base + RING + i), 0)[1], 0)
        return 0

    lax.fori_loop(0, n_up, gated, 0)

    def d2d2(n):
        return remote(ds2.at[n], dr2.at[n], d2s.at[n], d2r.at[n], z, other)

    def rs2(n, i):
        off = offsets[i]
        return remote(ss2.at[n, away(off)], sr2.at[n, slot_of(off)], r2s.at[n, i], r2r.at[n], away(off), c)

    def pass_on2(n):
        d2d2(n).wait_recv()
        t = own2[n] + dr2[n].astype(F32)
        own2[n] = t
        for a in range(chips):
            ss2[n, a] = t[a * BLOCK : (a + 1) * BLOCK].astype(BF16)
        for i in range(chips - 1):
            rs2(n, i).start()

    def down(n, _):
        for e in range(2):
            slot = lax.rem(first_down + 2 * n + e, RING)
            ready_rows(wd, hidden, slot)
            t = jnp.dot(hid[...], slots[slot, :hidden, :], preferred_element_type=F32)
            if e == 0:
                ds2[n] = t.astype(BF16)
                d2d2(n).start()
            else:
                own2[n] = t

        @pl.when(n > 0)
        def _():
            pass_on2(n - 1)

        return 0

    lax.fori_loop(0, n_down, down, 0)
    pass_on2(n_down - 1)

    def ag2(n, i):
        off = offsets[i]
        return remote(yb.at[n, c, z], yb.at[n, c, z], a2s.at[n, i], a2r.at[n], away(off), c)

    def fw2(n):
        return remote(yb.at[n, c], yb.at[n, c], f2s.at[n], f2r.at[n], z, other)

    def finished(n, _):
        arrived(sr2.at[n], r2r.at[n])
        t = own2[n, pl.ds(pl.multiple_of(z * BLOCK, BLOCK), BLOCK), :]
        for a in range(chips - 1):
            t = t + sr2[n, a].astype(F32)
        t = t + hb[z, c, :, pl.ds(pl.multiple_of(n * CHUNK, CHUNK), CHUNK)].astype(F32)
        yb[n, c, z] = t.astype(BF16)
        for i in range(chips - 1):
            ag2(n, i).start()
        return 0

    lax.fori_loop(0, n_down, finished, 0)

    def forward(n, _):
        arrived(yb.at[n, c, pl.ds(0, chips - 1)], a2r.at[n])
        fw2(n).start()
        return 0

    lax.fori_loop(0, n_down, forward, 0)

    def result(n, _):
        arrived(yb.at[n, other], f2r.at[n])
        pltpu.make_async_copy(yb.at[n], out.at[n], out_sem.at[n]).start()
        return 0

    lax.fori_loop(0, n_down, result, 0)

    def sent1(j, _):
        d2d1(j).wait_send()

        @pl.when(j < chips - 1)
        def _():
            rs1(j).wait_send()

        return 0

    lax.fori_loop(0, chips, sent1, 0)
    for i in range(chips - 1):
        ag1(i).wait_send()
        fw1(1 + i, away(offsets[i])).wait_send()
    fw1(0, z).wait_send()

    def sent2(n, _):
        d2d2(n).wait_send()
        for i in range(chips - 1):
            rs2(n, i).wait_send()
            ag2(n, i).wait_send()
        fw2(n).wait_send()
        pltpu.make_async_copy(yb.at[n], out.at[n], out_sem.at[n]).wait()
        return 0

    lax.fori_loop(0, n_down, sent2, 0)


def solution(mesh):
    chips = mesh.shape["tp"] // CORES

    def step(x, k_cache, v_cache, gain_a, wq, wo, gain_m, w_gate, w_up, w_down):
        batch, cache = k_cache.shape[:2]
        d, hidden = x.shape[1], w_down.shape[0]
        half = d // CORES
        k, v = (t.reshape(batch, cache, HEAD) for t in (k_cache, v_cache))
        gains = jnp.stack([gain_a, gain_m]).astype(F32)
        rot = jnp.asarray(turns(cache - 1))
        rows, n_down, peers = max(half, cache, hidden), half // CHUNK, chips - 1
        vmem, dma = pltpu.VMEM, pltpu.SemaphoreType.DMA
        y = pl.pallas_call(
            functools.partial(layer, chips),
            out_shape=jax.ShapeDtypeStruct((n_down, CORES, chips, BLOCK, CHUNK), BF16),
            in_specs=[pl.BlockSpec(memory_space=pl.ANY)] * 10,
            out_specs=pl.BlockSpec(memory_space=pl.ANY),
            scratch_shapes=[
                vmem((RING, rows, CHUNK), BF16),
                vmem(wq.shape, BF16),
                vmem((2, wo.shape[0], half), BF16),
                vmem((2, d), F32),
                vmem((2, HEAD), F32),
                vmem((chips, CORES, BLOCK, half), BF16),
                vmem((chips, CORES, BLOCK, half), BF16),
                vmem((CORES, batch, half), BF16),
                vmem((chips, 2 * BLOCK, HEAD), BF16),
                vmem((batch, hidden), BF16),
                vmem((chips, BLOCK, half), F32),
                vmem((chips, BLOCK, half), BF16),
                vmem((chips, BLOCK, half), BF16),
                vmem((chips, BLOCK, half), BF16),
                vmem((peers, BLOCK, half), BF16),
                vmem((n_down, batch, CHUNK), F32),
                vmem((n_down, batch, CHUNK), BF16),
                vmem((n_down, batch, CHUNK), BF16),
                vmem((n_down, chips, BLOCK, CHUNK), BF16),
                vmem((n_down, peers, BLOCK, CHUNK), BF16),
                vmem((n_down, CORES, chips, BLOCK, CHUNK), BF16),
                dma((RING, 2)),
                dma((6,)),
                dma((chips,)), dma((chips,)), dma((chips,)), dma, dma((peers,)), dma((peers,)), dma((chips,)), dma,
                dma((n_down,)), dma((n_down,)), dma((n_down, peers)), dma((n_down,)), dma((n_down, peers)), dma((n_down,)),
                dma((n_down,)), dma((n_down,)), dma((n_down,)),
            ],
            compiler_params=pltpu.CompilerParams(collective_id=0, has_side_effects=True, vmem_limit_bytes=67_000_000),
            name="decoder_layer",
        )(x, k, v, gains, wq, wo, w_gate, w_up, w_down, rot)
        return y.transpose(2, 3, 1, 0, 4).reshape(batch, d)

    states, cache, columns, rows_of = P("dp", None), P("dp", None, "tp", None), P(None, "tp"), P("tp", None)
    return jax.shard_map(
        step,
        mesh=mesh,
        in_specs=(states, cache, cache, P(None), columns, rows_of, P(None), columns, columns, rows_of),
        out_specs=states,
        check_vma=False,
    )
```

```python
import functools

import jax
import jax.numpy as jnp
import numpy as np
from jax import lax
from jax.experimental import pallas as pl
from jax.experimental.pallas import tpu as pltpu
from jax.sharding import PartitionSpec as P

HEAD = 128
THETA = 10000
CHUNK = 256
RING = 40
BLOCK = 8
CORES = 2
F32, BF16 = jnp.float32, jnp.bfloat16
MESH = pl.DeviceIdType.MESH


def turns(place):
    half = HEAD // 2
    angle = np.float64(place) * np.float64(THETA) ** (-np.arange(half) / half)
    cos, sin = np.cos(angle), np.sin(angle)
    return np.stack([np.concatenate([cos, cos]), np.concatenate([-sin, sin])]).astype(np.float32)


def layer(chips, x, k, v, gain_a, gain_m, wq, wo, wg, wu, wd, rot, out, slots, wq_v, wo_v, gain_a_v, gain_m_v, rot_v, xb, hb, bb, qb, hid,
          own1, ds1, dr1, ss1, sr1, own2, ds2, dr2, ss2, sr2, yb,
          ring_sem, misc_sem, d1s, d1r, r1s, r1r, a1s, a1r, f1s, f1r, d2s, d2r, r2s, r2r, a2s, a2r, f2s, f2r, out_sem):
    d = wq.shape[0]
    half = d // CORES
    cache = k.shape[1]
    hidden = wd.shape[0]
    pairs = BLOCK // 2
    per_block = 2 * pairs
    n_kv = chips * per_block
    n_up = hidden // CHUNK
    n_down = half // CHUNK
    first_down = n_kv + 4 * n_up

    me = lax.axis_index("tp")
    z, c = me // CORES, lax.rem(me, CORES)
    other = 1 - c
    offsets = [chips // 2]
    for far in range(chips // 2 - 1, 0, -1):
        offsets += [far, -far]

    def device(chip, core):
        return {"tp": chip * CORES + core}

    def away(off):
        return lax.rem(z + off + chips, chips)

    def slot_of(off):
        return (-off) % chips - 1

    def dest(j):
        far = chips // 2 - (j + 1) // 2
        return lax.rem(z + jnp.where(lax.rem(j, 2) == 1, far, chips - far), chips)

    def remote(src, dst, send, recv, chip, core):
        return pltpu.make_async_remote_copy(src_ref=src, dst_ref=dst, send_sem=send, recv_sem=recv, device_id=device(chip, core), device_id_type=MESH)

    def arrived(ref, sem):
        pltpu.make_async_copy(ref, ref, sem).wait()

    blocks = RING // per_block

    def slot(first, i):
        at = first % RING + i
        return jnp.where(at >= RING, at - RING, at)

    def fill_cache(j, s):
        row0 = dest(j) * BLOCK
        for w in range(per_block):
            src = k if w < pairs else v
            for e in range(2):
                pltpu.make_async_copy(
                    src.at[row0 + 2 * (w % pairs) + e], slots.at[s + w, pl.ds(0, cache), pl.ds(e * HEAD, HEAD)], ring_sem.at[s + w]
                ).start()

    def fill_up(n, s):
        columns = pl.ds(pl.multiple_of(n * CHUNK, CHUNK), CHUNK)
        for r in range(4):
            src = wg if r < 2 else wu
            pltpu.make_async_copy(src.at[pl.ds(r % 2 * half, half), columns], slots.at[s + r, pl.ds(0, half), :], ring_sem.at[s + r]).start()

    def fill_down(n, s):
        for e, core in enumerate((other, c)):
            columns = pl.ds(pl.multiple_of(core * half + n * CHUNK, CHUNK), CHUNK)
            pltpu.make_async_copy(wd.at[:, columns], slots.at[s + e, pl.ds(0, hidden), :], ring_sem.at[s + e]).start()

    def fill_weights(n, s):
        @pl.when(n < n_up)
        def _():
            fill_up(n, s)

        for e in range(2):
            m = 2 * (n - n_up) + e

            @pl.when((m >= 0) & (m < n_down))
            def _():
                fill_down(m, s + 2 * e)

    def ready(s, rows):
        arrived(slots.at[s, pl.ds(0, rows), :], ring_sem.at[s])

    def x_copy(a, b):
        return pltpu.make_async_copy(x.at[pl.ds(a * BLOCK, BLOCK), pl.ds(b * half, half)], xb.at[a, b], misc_sem.at[0])

    for a in range(chips):
        for b in range(CORES):
            x_copy(a, b).start()
    small = [pltpu.make_async_copy(src, dst, misc_sem.at[1 + i]) for i, (src, dst) in enumerate(((gain_a, gain_a_v), (gain_m, gain_m_v), (rot, rot_v), (wq, wq_v)))]
    for copy in small:
        copy.start()

    barrier = pltpu.get_barrier_semaphore()
    for off in offsets:
        pl.semaphore_signal(barrier, inc=1, device_id=device(away(off), c), device_id_type=MESH)
    pl.semaphore_signal(barrier, inc=1, device_id=device(z, other), device_id_type=MESH)

    def normed(src, which):
        gain = which[...].astype(F32).reshape(1, d)

        def two_blocks(m, _):
            rows = [[src[2 * m + a, b].astype(F32) for b in range(CORES)] for a in range(2)]
            scaled = []
            for parts in rows:
                mean = sum(jnp.sum(t * t, -1, keepdims=True) for t in parts) / d
                scale = lax.rsqrt(mean + 1e-6)
                scaled.append([t * scale * gain[:, b * half : (b + 1) * half] for b, t in enumerate(parts)])
            at = pl.ds(pl.multiple_of(m * 2 * BLOCK, 2 * BLOCK), 2 * BLOCK)
            for b in range(CORES):
                bb[b, at, :] = jnp.concatenate([scaled[0][b], scaled[1][b]], 0).astype(BF16)
            return 0

        lax.fori_loop(0, chips // 2, two_blocks, 0)

    arrived(xb, misc_sem.at[0])

    def fill_first(j, _):
        fill_cache(j, j * per_block)
        return 0

    lax.fori_loop(0, 1, fill_first, 0)
    wo_copies = [
        pltpu.make_async_copy(wo.at[:, pl.ds(pl.multiple_of(core * half, CHUNK), half)], wo_v.at[e], misc_sem.at[5 + e])
        for e, core in enumerate((other, c))
    ]
    for copy in wo_copies:
        copy.start()
    lax.fori_loop(1, blocks, fill_first, 0)
    for a in range(3):
        small[a].wait()
    normed(xb, gain_a_v)
    small[3].wait()
    q = jnp.dot(bb[0], wq_v[:half], preferred_element_type=F32) + jnp.dot(bb[1], wq_v[half:], preferred_element_type=F32)
    q = q.astype(BF16).astype(F32)
    turned = []
    for h in range(2):
        t = q[:, h * HEAD : (h + 1) * HEAD]
        turned.append(t * rot_v[0:1, :] + pltpu.roll(t, HEAD // 2, 1) * rot_v[1:2, :])
    for a in range(chips):
        rows = slice(a * BLOCK, (a + 1) * BLOCK)
        qb[a] = jnp.concatenate([turned[0][rows], turned[1][rows]], 0).astype(BF16)
    for copy in wo_copies:
        copy.wait()

    row = lax.rem(lax.broadcasted_iota(jnp.int32, (2 * BLOCK, 2 * HEAD), 0), BLOCK)
    side = lax.broadcasted_iota(jnp.int32, (2 * BLOCK, 2 * HEAD), 1) // HEAD

    def d2d1(j):
        return remote(ds1.at[j], dr1.at[j], d1s.at[j], d1r.at[j], z, other)

    def rs1(j):
        t = dest(j)
        return remote(ss1.at[j], sr1.at[lax.rem(z - t + chips, chips) - 1], r1s.at[j], r1r, t, c)

    def pass_on(j):
        d2d1(j).wait_recv()
        ss1[j] = (own1[j] + dr1[j].astype(F32)).astype(BF16)
        rs1(j).start()

    def attend(j, _):
        base = slot(0, j * per_block)
        q16 = qb[dest(j)]
        wide = jnp.concatenate([q16, q16], 1)
        for p in range(pairs):
            ready(base + p, cache)
        s = None
        for p in range(pairs):
            mine = jnp.where(row == 2 * p + side, wide, jnp.zeros_like(wide))
            part = lax.dot_general(mine, slots[base + p, :cache, :], (((1,), (1,)), ((), ())), preferred_element_type=F32)
            s = part if s is None else s + part
        s = s * HEAD**-0.5
        e = jnp.exp(s - jnp.max(s, -1, keepdims=True))
        weights = (e / jnp.sum(e, -1, keepdims=True)).astype(BF16)

        @pl.when(j == 0)
        def _():
            pl.semaphore_wait(barrier, len(offsets) + 1)

        @pl.when(j > 0)
        def _():
            pass_on(j - 1)

        for p in range(pairs):
            ready(base + pairs + p, cache)
        o = None
        for p in range(pairs):
            part = jnp.dot(weights, slots[base + pairs + p, :cache, :], preferred_element_type=F32)
            part = jnp.where(row == 2 * p + side, part, 0.0)
            o = part if o is None else o + part
        o = o[:, :HEAD] + o[:, HEAD:]
        seen = jnp.concatenate([o[:BLOCK], o[BLOCK:]], 1).astype(BF16)
        ds1[j] = jnp.dot(seen, wo_v[0], preferred_element_type=F32).astype(BF16)
        d2d1(j).start()
        own1[j] = jnp.dot(seen, wo_v[1], preferred_element_type=F32)

        @pl.when(j < chips - blocks)
        def _():
            fill_cache(j + blocks, base)

        @pl.when(j >= chips - blocks)
        def _():
            for e in range(2):
                fill_weights(2 * (j - (chips - blocks)) + e, base + 4 * e)

        return 0

    lax.fori_loop(0, chips, attend, 0)

    d2d1(chips - 1).wait_recv()
    h = own1[chips - 1] + dr1[chips - 1].astype(F32)
    arrived(sr1, r1r)
    for a in range(chips - 1):
        h = h + sr1[a].astype(F32)
    h = h + xb[z, c].astype(F32)
    hb[z, c] = h.astype(BF16)

    def ag1(i):
        off = offsets[i]
        return remote(hb.at[z, c], hb.at[z, c], a1s.at[i], a1r.at[slot_of(off)], away(off), c)

    def fw1(i, chip):
        return remote(hb.at[chip, c], hb.at[chip, c], f1s.at[i], f1r, z, other)

    for i in range(chips - 1):
        ag1(i).start()
    fw1(0, z).start()
    for i in reversed(range(chips - 1)):
        off = offsets[i]
        arrived(hb.at[away(off), c], a1r.at[off % chips - 1])
        fw1(1 + i, away(off)).start()
    arrived(hb.at[:, other], f1r)
    normed(hb, gain_m_v)

    def gated(n, _):
        base = slot(n_kv, 4 * n)
        for r in range(4):
            ready(base + r, half)
        parts = [jnp.dot(bb[r % 2], slots[base + r, :half, :], preferred_element_type=F32) for r in range(4)]
        gate, up = parts[0] + parts[1], parts[2] + parts[3]
        hid[:, pl.ds(pl.multiple_of(n * CHUNK, CHUNK), CHUNK)] = (gate * jax.nn.sigmoid(gate) * up).astype(BF16)
        fill_weights(n + 2 * blocks, base)
        return 0

    lax.fori_loop(0, n_up, gated, 0)

    def d2d2(n):
        return remote(ds2.at[n], dr2.at[n], d2s.at[n], d2r.at[n], z, other)

    def rs2(n, i):
        off = offsets[i]
        return remote(ss2.at[n, away(off)], sr2.at[n, slot_of(off)], r2s.at[n, i], r2r.at[n], away(off), c)

    def pass_on2(n):
        d2d2(n).wait_recv()
        t = own2[n] + dr2[n].astype(F32)
        own2[n] = t
        for a in range(chips):
            ss2[n, a] = t[a * BLOCK : (a + 1) * BLOCK].astype(BF16)
        for i in range(chips - 1):
            rs2(n, i).start()

    def down(n, _):
        for e in range(2):
            at = slot(first_down, 2 * n) + e
            ready(at, hidden)
            t = jnp.dot(hid[...], slots[at, :hidden, :], preferred_element_type=F32)
            if e == 0:
                ds2[n] = t.astype(BF16)
                d2d2(n).start()
            else:
                own2[n] = t

        @pl.when(n > 0)
        def _():
            pass_on2(n - 1)

        return 0

    lax.fori_loop(0, n_down, down, 0)
    pass_on2(n_down - 1)

    def ag2(n, i):
        off = offsets[i]
        return remote(yb.at[n, c, z], yb.at[n, c, z], a2s.at[n, i], a2r.at[n], away(off), c)

    def fw2(n):
        return remote(yb.at[n, c], yb.at[n, c], f2s.at[n], f2r.at[n], z, other)

    def finished(n, _):
        arrived(sr2.at[n], r2r.at[n])
        t = own2[n, pl.ds(pl.multiple_of(z * BLOCK, BLOCK), BLOCK), :]
        for a in range(chips - 1):
            t = t + sr2[n, a].astype(F32)
        t = t + hb[z, c, :, pl.ds(pl.multiple_of(n * CHUNK, CHUNK), CHUNK)].astype(F32)
        yb[n, c, z] = t.astype(BF16)
        for i in range(chips - 1):
            ag2(n, i).start()
        return 0

    lax.fori_loop(0, n_down, finished, 0)

    def forward(n, _):
        arrived(yb.at[n, c, pl.ds(0, chips - 1)], a2r.at[n])
        fw2(n).start()
        return 0

    lax.fori_loop(0, n_down, forward, 0)

    def result(n, _):
        arrived(yb.at[n, other], f2r.at[n])
        pltpu.make_async_copy(yb.at[n], out.at[n], out_sem.at[n]).start()
        return 0

    lax.fori_loop(0, n_down, result, 0)

    def sent1(j, _):
        d2d1(j).wait_send()

        @pl.when(j < chips - 1)
        def _():
            rs1(j).wait_send()

        return 0

    lax.fori_loop(0, chips, sent1, 0)
    for i in range(chips - 1):
        ag1(i).wait_send()
        fw1(1 + i, away(offsets[i])).wait_send()
    fw1(0, z).wait_send()

    def sent2(n, _):
        d2d2(n).wait_send()
        for i in range(chips - 1):
            rs2(n, i).wait_send()
            ag2(n, i).wait_send()
        fw2(n).wait_send()
        pltpu.make_async_copy(yb.at[n], out.at[n], out_sem.at[n]).wait()
        return 0

    lax.fori_loop(0, n_down, sent2, 0)


def solution(mesh):
    chips = mesh.shape["tp"] // CORES

    def step(x, k_cache, v_cache, gain_a, wq, wo, gain_m, w_gate, w_up, w_down):
        batch, cache = k_cache.shape[:2]
        d, hidden = x.shape[1], w_down.shape[0]
        half = d // CORES
        k, v = (t.reshape(batch, cache, HEAD) for t in (k_cache, v_cache))
        rot = jnp.asarray(turns(cache - 1))
        rows, n_down, peers = max(half, cache, hidden), half // CHUNK, chips - 1
        vmem, dma = pltpu.VMEM, pltpu.SemaphoreType.DMA
        y = pl.pallas_call(
            functools.partial(layer, chips),
            out_shape=jax.ShapeDtypeStruct((n_down, CORES, chips, BLOCK, CHUNK), BF16),
            in_specs=[pl.BlockSpec(memory_space=pl.ANY)] * 11,
            out_specs=pl.BlockSpec(memory_space=pl.ANY),
            scratch_shapes=[
                vmem((RING, rows, CHUNK), BF16),
                vmem(wq.shape, BF16),
                vmem((2, wo.shape[0], half), BF16),
                vmem((d,), BF16),
                vmem((d,), BF16),
                vmem((2, HEAD), F32),
                vmem((chips, CORES, BLOCK, half), BF16),
                vmem((chips, CORES, BLOCK, half), BF16),
                vmem((CORES, batch, half), BF16),
                vmem((chips, 2 * BLOCK, HEAD), BF16),
                vmem((batch, hidden), BF16),
                vmem((chips, BLOCK, half), F32),
                vmem((chips, BLOCK, half), BF16),
                vmem((chips, BLOCK, half), BF16),
                vmem((chips, BLOCK, half), BF16),
                vmem((peers, BLOCK, half), BF16),
                vmem((n_down, batch, CHUNK), F32),
                vmem((n_down, batch, CHUNK), BF16),
                vmem((n_down, batch, CHUNK), BF16),
                vmem((n_down, chips, BLOCK, CHUNK), BF16),
                vmem((n_down, peers, BLOCK, CHUNK), BF16),
                vmem((n_down, CORES, chips, BLOCK, CHUNK), BF16),
                dma((RING,)),
                dma((7,)),
                dma((chips,)), dma((chips,)), dma((chips,)), dma, dma((peers,)), dma((peers,)), dma((chips,)), dma,
                dma((n_down,)), dma((n_down,)), dma((n_down, peers)), dma((n_down,)), dma((n_down, peers)), dma((n_down,)),
                dma((n_down,)), dma((n_down,)), dma((n_down,)),
            ],
            compiler_params=pltpu.CompilerParams(collective_id=0, has_side_effects=True, vmem_limit_bytes=67_000_000),
            name="decoder_layer",
        )(x, k, v, gain_a, gain_m, wq, wo, w_gate, w_up, w_down, rot)
        return y.transpose(2, 3, 1, 0, 4).reshape(batch, d)

    states, cache, columns, rows_of = P("dp", None), P("dp", None, "tp", None), P(None, "tp"), P("tp", None)
    return jax.shard_map(
        step,
        mesh=mesh,
        in_specs=(states, cache, cache, P(None), columns, rows_of, P(None), columns, columns, rows_of),
        out_specs=states,
        check_vma=False,
    )
```

```python
import functools

import jax
import jax.numpy as jnp
import numpy as np
from jax import lax
from jax.experimental import pallas as pl
from jax.experimental.pallas import tpu as pltpu
from jax.sharding import PartitionSpec as P

HEAD = 128
THETA = 10000
CHUNK = 256
RING = 40
BLOCK = 8
CORES = 2
F32, BF16 = jnp.float32, jnp.bfloat16
MESH = pl.DeviceIdType.MESH


def turns(place):
    half = HEAD // 2
    angle = np.float64(place) * np.float64(THETA) ** (-np.arange(half) / half)
    cos, sin = np.cos(angle), np.sin(angle)
    return np.stack([np.concatenate([cos, cos]), np.concatenate([-sin, sin])]).astype(np.float32)


def layer(chips, x, k, v, gain_a, gain_m, wq, wo, wg, wu, wd, rot, out, slots, wq_v, wo_v, gain_a_v, gain_m_v, rot_v, xb, hb, bb, qb, hid,
          own1, ds1, dr1, ss1, sr1, own2, ds2, dr2, ss2, sr2, yb,
          ring_sem, misc_sem, d1s, d1r, r1s, r1r, a1s, a1r, f1s, f1r, d2s, d2r, r2s, r2r, a2s, a2r, f2s, f2r, out_sem):
    d = wq.shape[0]
    half = d // CORES
    cache = k.shape[1]
    hidden = wd.shape[0]
    pairs = BLOCK // 2
    per_block = 2 * pairs
    n_kv = chips * per_block
    n_up = hidden // CHUNK
    n_down = half // CHUNK
    first_down = n_kv + 4 * n_up

    me = lax.axis_index("tp")
    z, c = me // CORES, lax.rem(me, CORES)
    other = 1 - c
    offsets = [chips // 2]
    for far in range(chips // 2 - 1, 0, -1):
        offsets += [far, -far]

    def device(chip, core):
        return {"tp": chip * CORES + core}

    def away(off):
        return lax.rem(z + off + chips, chips)

    def slot_of(off):
        return (-off) % chips - 1

    def dest(j):
        far = chips // 2 - (j + 1) // 2
        return lax.rem(z + jnp.where(lax.rem(j, 2) == 1, far, chips - far), chips)

    def remote(src, dst, send, recv, chip, core):
        return pltpu.make_async_remote_copy(src_ref=src, dst_ref=dst, send_sem=send, recv_sem=recv, device_id=device(chip, core), device_id_type=MESH)

    def arrived(ref, sem):
        pltpu.make_async_copy(ref, ref, sem).wait()

    blocks = RING // per_block

    def slot(first, i):
        at = first % RING + i
        return jnp.where(at >= RING, at - RING, at)

    def fill_cache(j, s):
        row0 = dest(j) * BLOCK
        for w in range(per_block):
            src = k if w < pairs else v
            for e in range(2):
                pltpu.make_async_copy(
                    src.at[row0 + 2 * (w % pairs) + e], slots.at[s + w, pl.ds(0, cache), pl.ds(e * HEAD, HEAD)], ring_sem.at[s + w]
                ).start()

    def fill_up(n, s):
        columns = pl.ds(pl.multiple_of(n * CHUNK, CHUNK), CHUNK)
        for r in range(4):
            src = wg if r < 2 else wu
            pltpu.make_async_copy(src.at[pl.ds(r % 2 * half, half), columns], slots.at[s + r, pl.ds(0, half), :], ring_sem.at[s + r]).start()

    def fill_down(n, s):
        for e, core in enumerate((other, c)):
            columns = pl.ds(pl.multiple_of(core * half + n * CHUNK, CHUNK), CHUNK)
            pltpu.make_async_copy(wd.at[:, columns], slots.at[s + e, pl.ds(0, hidden), :], ring_sem.at[s + e]).start()

    def fill_weights(n, s):
        @pl.when(n < n_up)
        def _():
            fill_up(n, s)

        for e in range(2):
            m = 2 * (n - n_up) + e

            @pl.when((m >= 0) & (m < n_down))
            def _():
                fill_down(m, s + 2 * e)

    def ready(s, rows):
        arrived(slots.at[s, pl.ds(0, rows), :], ring_sem.at[s])

    def x_copy(a, b):
        return pltpu.make_async_copy(x.at[pl.ds(a * BLOCK, BLOCK), pl.ds(b * half, half)], xb.at[a, b], misc_sem.at[0])

    for a in range(chips):
        for b in range(CORES):
            x_copy(a, b).start()
    small = [pltpu.make_async_copy(src, dst, misc_sem.at[1 + i]) for i, (src, dst) in enumerate(((gain_a, gain_a_v), (gain_m, gain_m_v), (rot, rot_v), (wq, wq_v)))]
    for copy in small:
        copy.start()

    def fill_first(j, _):
        fill_cache(j, j * per_block)
        return 0

    lax.fori_loop(0, 1, fill_first, 0)
    wo_copies = [
        pltpu.make_async_copy(wo.at[:, pl.ds(pl.multiple_of(core * half, CHUNK), half)], wo_v.at[e], misc_sem.at[5 + e])
        for e, core in enumerate((other, c))
    ]
    for copy in wo_copies:
        copy.start()
    lax.fori_loop(1, blocks, fill_first, 0)

    barrier = pltpu.get_barrier_semaphore()
    for off in offsets:
        pl.semaphore_signal(barrier, inc=1, device_id=device(away(off), c), device_id_type=MESH)
    pl.semaphore_signal(barrier, inc=1, device_id=device(z, other), device_id_type=MESH)

    def normed(src, which):
        gain = which[...].astype(F32).reshape(1, d)

        def two_blocks(m, _):
            rows = [[src[2 * m + a, b].astype(F32) for b in range(CORES)] for a in range(2)]
            scaled = []
            for parts in rows:
                mean = sum(jnp.sum(t * t, -1, keepdims=True) for t in parts) / d
                scale = lax.rsqrt(mean + 1e-6)
                scaled.append([t * scale * gain[:, b * half : (b + 1) * half] for b, t in enumerate(parts)])
            at = pl.ds(pl.multiple_of(m * 2 * BLOCK, 2 * BLOCK), 2 * BLOCK)
            for b in range(CORES):
                bb[b, at, :] = jnp.concatenate([scaled[0][b], scaled[1][b]], 0).astype(BF16)
            return 0

        lax.fori_loop(0, chips // 2, two_blocks, 0)

    arrived(xb, misc_sem.at[0])
    for a in range(3):
        small[a].wait()
    normed(xb, gain_a_v)
    small[3].wait()
    q = jnp.dot(bb[0], wq_v[:half], preferred_element_type=F32) + jnp.dot(bb[1], wq_v[half:], preferred_element_type=F32)
    q = q.astype(BF16).astype(F32)
    turned = []
    for h in range(2):
        t = q[:, h * HEAD : (h + 1) * HEAD]
        turned.append(t * rot_v[0:1, :] + pltpu.roll(t, HEAD // 2, 1) * rot_v[1:2, :])
    for a in range(chips):
        rows = slice(a * BLOCK, (a + 1) * BLOCK)
        qb[a] = jnp.concatenate([turned[0][rows], turned[1][rows]], 0).astype(BF16)
    for copy in wo_copies:
        copy.wait()

    row = lax.rem(lax.broadcasted_iota(jnp.int32, (2 * BLOCK, 2 * HEAD), 0), BLOCK)
    side = lax.broadcasted_iota(jnp.int32, (2 * BLOCK, 2 * HEAD), 1) // HEAD

    def d2d1(j):
        return remote(ds1.at[j], dr1.at[j], d1s, d1r.at[j], z, other)

    def rs1(j):
        t = dest(j)
        return remote(ss1.at[j], sr1.at[lax.rem(z - t + chips, chips) - 1], r1s, r1r, t, c)

    def pass_on(j):
        d2d1(j).wait_recv()
        ss1[j] = (own1[j] + dr1[j].astype(F32)).astype(BF16)
        rs1(j).start()

    def attend(j, _):
        base = slot(0, j * per_block)
        q16 = qb[dest(j)]
        wide = jnp.concatenate([q16, q16], 1)
        for p in range(pairs):
            ready(base + p, cache)
        s = None
        for p in range(pairs):
            mine = jnp.where(row == 2 * p + side, wide, jnp.zeros_like(wide))
            part = lax.dot_general(mine, slots[base + p, :cache, :], (((1,), (1,)), ((), ())), preferred_element_type=F32)
            s = part if s is None else s + part
        s = s * HEAD**-0.5
        e = jnp.exp(s - jnp.max(s, -1, keepdims=True))
        weights = (e / jnp.sum(e, -1, keepdims=True)).astype(BF16)

        @pl.when(j == 0)
        def _():
            pl.semaphore_wait(barrier, len(offsets) + 1)

        @pl.when(j > 0)
        def _():
            pass_on(j - 1)

        for p in range(pairs):
            ready(base + pairs + p, cache)
        o = None
        for p in range(pairs):
            part = jnp.dot(weights, slots[base + pairs + p, :cache, :], preferred_element_type=F32)
            part = jnp.where(row == 2 * p + side, part, 0.0)
            o = part if o is None else o + part
        o = o[:, :HEAD] + o[:, HEAD:]
        seen = jnp.concatenate([o[:BLOCK], o[BLOCK:]], 1).astype(BF16)
        ds1[j] = jnp.dot(seen, wo_v[0], preferred_element_type=F32).astype(BF16)
        d2d1(j).start()
        own1[j] = jnp.dot(seen, wo_v[1], preferred_element_type=F32)

        @pl.when(j < chips - blocks)
        def _():
            fill_cache(j + blocks, base)

        @pl.when(j >= chips - blocks)
        def _():
            for e in range(2):
                fill_weights(2 * (j - (chips - blocks)) + e, base + 4 * e)

        return 0

    lax.fori_loop(0, chips, attend, 0)

    d2d1(chips - 1).wait_recv()
    h = own1[chips - 1] + dr1[chips - 1].astype(F32)
    arrived(sr1, r1r)
    for a in range(chips - 1):
        h = h + sr1[a].astype(F32)
    h = h + xb[z, c].astype(F32)
    hb[z, c] = h.astype(BF16)

    def ag1(i):
        off = offsets[i]
        return remote(hb.at[z, c], hb.at[z, c], a1s, a1r.at[slot_of(off)], away(off), c)

    def fw1(chip):
        return remote(hb.at[chip, c], hb.at[chip, c], f1s, f1r, z, other)

    for i in range(chips - 1):
        ag1(i).start()
    fw1(z).start()
    for i in reversed(range(chips - 1)):
        off = offsets[i]
        arrived(hb.at[away(off), c], a1r.at[off % chips - 1])
        fw1(away(off)).start()
    arrived(hb.at[:, other], f1r)
    normed(hb, gain_m_v)

    def gated(n, _):
        base = slot(n_kv, 4 * n)
        for r in range(4):
            ready(base + r, half)
        parts = [jnp.dot(bb[r % 2], slots[base + r, :half, :], preferred_element_type=F32) for r in range(4)]
        gate, up = parts[0] + parts[1], parts[2] + parts[3]
        hid[:, pl.ds(pl.multiple_of(n * CHUNK, CHUNK), CHUNK)] = (gate * jax.nn.sigmoid(gate) * up).astype(BF16)
        fill_weights(n + 2 * blocks, base)
        return 0

    lax.fori_loop(0, n_up, gated, 0)

    def d2d2(n):
        return remote(ds2.at[n], dr2.at[n], d2s, d2r.at[n], z, other)

    def rs2(n, i):
        off = offsets[i]
        return remote(ss2.at[n, away(off)], sr2.at[n, slot_of(off)], r2s, r2r.at[n], away(off), c)

    def pass_on2(n):
        d2d2(n).wait_recv()
        t = own2[n] + dr2[n].astype(F32)
        own2[n] = t
        for a in range(chips):
            ss2[n, a] = t[a * BLOCK : (a + 1) * BLOCK].astype(BF16)
        for i in range(chips - 1):
            rs2(n, i).start()

    def ag2(n, i):
        off = offsets[i]
        return remote(yb.at[n, z], yb.at[n, z], a2s, a2r.at[n], away(off), c)

    def finished(n):
        arrived(sr2.at[n], r2r.at[n])
        t = own2[n, pl.ds(pl.multiple_of(z * BLOCK, BLOCK), BLOCK), :]
        for a in range(chips - 1):
            t = t + sr2[n, a].astype(F32)
        t = t + hb[z, c, :, pl.ds(pl.multiple_of(n * CHUNK, CHUNK), CHUNK)].astype(F32)
        yb[n, z] = t.astype(BF16)
        for i in range(chips - 1):
            ag2(n, i).start()

    def down(n, _):
        for e in range(2):
            at = slot(first_down, 2 * n) + e
            ready(at, hidden)
            t = jnp.dot(hid[...], slots[at, :hidden, :], preferred_element_type=F32)
            if e == 0:
                ds2[n] = t.astype(BF16)
                d2d2(n).start()
            else:
                own2[n] = t

        @pl.when(n > 0)
        def _():
            pass_on2(n - 1)

        return 0

    lax.fori_loop(0, n_down, down, 0)
    pass_on2(n_down - 1)
    lax.fori_loop(0, n_down, lambda n, _: (finished(n), 0)[1], 0)

    def columns_of(core, n):
        return out.at[:, :, pl.ds(pl.multiple_of(core * half + n * CHUNK, CHUNK), CHUNK)]

    def kept(n):
        return pltpu.make_async_copy(yb.at[n], columns_of(c, n), out_sem)

    def fw2(n):
        return remote(yb.at[n], columns_of(c, n), f2s, f2r, z, other)

    def forward(n, _):
        arrived(yb.at[n, pl.ds(0, chips - 1)], a2r.at[n])
        fw2(n).start()
        kept(n).start()
        return 0

    lax.fori_loop(0, n_down, forward, 0)

    arrived(ds1, d1s)
    arrived(sr1, r1s)
    arrived(sr1, a1s)
    arrived(ds1, f1s)
    arrived(ds2, d2s)
    arrived(sr2, r2s)
    arrived(sr2, a2s)
    arrived(yb, f2s)
    arrived(yb, out_sem)
    arrived(yb, f2r)


def solution(mesh):
    chips = mesh.shape["tp"] // CORES

    def step(x, k_cache, v_cache, gain_a, wq, wo, gain_m, w_gate, w_up, w_down):
        batch, cache = k_cache.shape[:2]
        d, hidden = x.shape[1], w_down.shape[0]
        half = d // CORES
        k, v = (t.reshape(batch, cache, HEAD) for t in (k_cache, v_cache))
        rot = jnp.asarray(turns(cache - 1))
        rows, n_down, peers = max(half, cache, hidden), half // CHUNK, chips - 1
        vmem, dma = pltpu.VMEM, pltpu.SemaphoreType.DMA
        y = pl.pallas_call(
            functools.partial(layer, chips),
            out_shape=jax.ShapeDtypeStruct((chips, BLOCK, d), BF16),
            in_specs=[pl.BlockSpec(memory_space=pl.ANY)] * 11,
            out_specs=pl.BlockSpec(memory_space=pl.ANY),
            scratch_shapes=[
                vmem((RING, rows, CHUNK), BF16),
                vmem(wq.shape, BF16),
                vmem((2, wo.shape[0], half), BF16),
                vmem((d,), BF16),
                vmem((d,), BF16),
                vmem((2, HEAD), F32),
                vmem((chips, CORES, BLOCK, half), BF16),
                vmem((chips, CORES, BLOCK, half), BF16),
                vmem((CORES, batch, half), BF16),
                vmem((chips, 2 * BLOCK, HEAD), BF16),
                vmem((batch, hidden), BF16),
                vmem((chips, BLOCK, half), F32),
                vmem((chips, BLOCK, half), BF16),
                vmem((chips, BLOCK, half), BF16),
                vmem((chips, BLOCK, half), BF16),
                vmem((peers, BLOCK, half), BF16),
                vmem((n_down, batch, CHUNK), F32),
                vmem((n_down, batch, CHUNK), BF16),
                vmem((n_down, batch, CHUNK), BF16),
                vmem((n_down, chips, BLOCK, CHUNK), BF16),
                vmem((n_down, peers, BLOCK, CHUNK), BF16),
                vmem((n_down, chips, BLOCK, CHUNK), BF16),
                dma((RING,)),
                dma((7,)),
                dma, dma((chips,)), dma, dma, dma, dma((peers,)), dma, dma,
                dma, dma((n_down,)), dma, dma((n_down,)), dma, dma((n_down,)), dma, dma, dma,
            ],
            compiler_params=pltpu.CompilerParams(collective_id=0, has_side_effects=True, vmem_limit_bytes=67_000_000),
            name="decoder_layer",
        )(x, k, v, gain_a, gain_m, wq, wo, w_gate, w_up, w_down, rot)
        return y.reshape(batch, d)

    states, cache, columns, rows_of = P("dp", None), P("dp", None, "tp", None), P(None, "tp"), P("tp", None)
    return jax.shard_map(
        step,
        mesh=mesh,
        in_specs=(states, cache, cache, P(None), columns, rows_of, P(None), columns, columns, rows_of),
        out_specs=states,
        check_vma=False,
    )
```
